16 devices in a mesh: dp: 2 (over y, z), tp: 8 (over x, core).
Axes of the slice: x: 4, y: 2, z: 1, core: 2. Of those that a mesh axis runs over, the one named last changes fastest.
The devices are a block of a 4x4x8 slice.
Arguments:
- tokens: bfloat16 [4, 1024, 4096], P('dp', 'tp'), parts along dimension 0
- pad_mask: int32 [4, 1024], P('dp'), parts along dimension 0
- rel_table: float32 [32, 64], P(None, 'tp')
- w_query: bfloat16 [2, 4096, 4096], P(None, None, 'tp')
- w_key: bfloat16 [2, 4096, 4096], P(None, None, 'tp')
- w_value: bfloat16 [2, 4096, 4096], P(None, None, 'tp')
- w_out: bfloat16 [2, 4096, 4096], P(None, 'tp')
- w_act: bfloat16 [2, 4096, 10240], P(None, None, 'tp')
- w_lin: bfloat16 [2, 4096, 10240], P(None, None, 'tp')
- w_down: bfloat16 [2, 10240, 4096], P(None, 'tp')
- norm_attn: float32 [2, 4096], replicated
- norm_mlp: float32 [2, 4096], replicated
Outputs:
- output: bfloat16 [4, 1024, 4096], P('dp', 'tp'), parts along dimension 0
There are 2 independent parts. The reference program is written for one: setup_inputs(seed, part) draws one part's arguments, and reference() takes and returns one part's arrays. A program takes and returns all parts, laid end to end along the dimension named above; an argument that names none is the same for every part.
All inputs are finite; a program needn't handle non-finite values.
Results may differ from the reference program's by a relative error of at most 0.02.
Values are sent between devices in bfloat16 or wider.
A program may use at most 768 MiB of HBM per device.

```python
import jax
import jax.numpy as jnp
from jax import lax

BATCH_SIZE = 2
SEQ_LEN = 1024
MODEL_DIM = 4096
NUM_HEADS = 64
HEAD_DIM = 64
FF_DIM = 10240
NUM_LAYERS = 2
NUM_BUCKETS = 32
INNER_DIM = NUM_HEADS * HEAD_DIM


def rel_bucket(offsets):
    side = jnp.where(offsets > 0, 16, 0)
    distance = jnp.minimum(jnp.abs(offsets), 128)
    limits = 64 * 2 ** jnp.arange(1, 8)
    steps = jnp.sum((distance[:, None] * distance[:, None] >= limits[None, :]).astype(jnp.int32), axis=1)
    return side + jnp.where(distance < 8, distance, 8 + steps)


def rms_norm(rows_in, gain_vec):
    rows32 = rows_in.astype(jnp.float32)
    inv_rms = lax.rsqrt(jnp.mean(rows32 * rows32, axis=-1, keepdims=True) + 1e-6)
    return (rows32 * inv_rms * gain_vec).astype(jnp.bfloat16)


def setup_inputs(seed: int = 0, part: int = 0) -> dict:
    root_key = jax.random.key(seed)
    subkeys = jax.random.split(root_key, 10)
    part_keys = jax.random.split(jax.random.fold_in(root_key, part), 3)

    def weight(rng_key, dims, fan_in, factor):
        normal_draw = jax.random.normal(rng_key, dims, jnp.float32)
        return (normal_draw * (factor * fan_in ** -0.5)).astype(jnp.bfloat16)

    tokens = jax.random.normal(part_keys[0], (BATCH_SIZE, SEQ_LEN, MODEL_DIM), jnp.float32).astype(jnp.bfloat16)
    lengths = jax.random.randint(part_keys[1], (BATCH_SIZE,), SEQ_LEN // 8, SEQ_LEN + 1)
    full_row = jax.random.randint(part_keys[2], (), 0, BATCH_SIZE)
    lengths = jnp.where(jnp.arange(BATCH_SIZE) == full_row, SEQ_LEN, lengths)
    pad_mask = (jnp.arange(SEQ_LEN)[None, :] < lengths[:, None]).astype(jnp.int32)
    attn_dims = (NUM_LAYERS, MODEL_DIM, INNER_DIM)
    ff_dims = (NUM_LAYERS, MODEL_DIM, FF_DIM)
    return {
        'tokens': tokens,
        'pad_mask': pad_mask,
        'rel_table': jax.random.normal(subkeys[0], (NUM_BUCKETS, NUM_HEADS), jnp.float32),
        'w_query': weight(subkeys[1], attn_dims, MODEL_DIM * HEAD_DIM, 2.5),
        'w_key': weight(subkeys[2], attn_dims, MODEL_DIM, 1.0),
        'w_value': weight(subkeys[3], attn_dims, MODEL_DIM, 1.0),
        'w_out': weight(subkeys[4], (NUM_LAYERS, INNER_DIM, MODEL_DIM), INNER_DIM, 1.0),
        'w_act': weight(subkeys[5], ff_dims, MODEL_DIM, 1.0),
        'w_lin': weight(subkeys[6], ff_dims, MODEL_DIM, 1.0),
        'w_down': weight(subkeys[7], (NUM_LAYERS, FF_DIM, MODEL_DIM), FF_DIM, 1.0),
        'norm_attn': jax.random.uniform(subkeys[8], (NUM_LAYERS, MODEL_DIM), jnp.float32, 0.5, 1.5),
        'norm_mlp': jax.random.uniform(subkeys[9], (NUM_LAYERS, MODEL_DIM), jnp.float32, 0.5, 1.5),
    }


def reference(tokens, pad_mask, rel_table, w_query, w_key, w_value, w_out, w_act, w_lin, w_down, norm_attn, norm_mlp):
    offsets = jnp.arange(2 * SEQ_LEN - 1) - (SEQ_LEN - 1)
    dist_table = rel_table[rel_bucket(offsets)]
    positions = jnp.arange(SEQ_LEN)
    index = positions[None, :] - positions[:, None] + (SEQ_LEN - 1)
    key_bias = jnp.where(pad_mask == 1, 0.0, -1e9).astype(jnp.float32)
    token_rows = BATCH_SIZE * SEQ_LEN

    def head_attn(operands):
        q_head, k_head, v_head, table_col = operands
        scores = jnp.einsum('bqe,bke->bqk', q_head.astype(jnp.float32), k_head.astype(jnp.float32))
        scores = scores + table_col[index][None] + key_bias[:, None, :]
        attn_probs = jax.nn.softmax(scores, axis=-1).astype(jnp.bfloat16)
        context = jnp.einsum('bqk,bke->bqe', attn_probs.astype(jnp.float32), v_head.astype(jnp.float32))
        return context.astype(jnp.bfloat16)

    def layer(residual, params):
        lay_query, lay_key, lay_value, lay_out, lay_act, lay_lin, lay_down, lay_norm1, lay_norm2 = params
        normed = rms_norm(residual, lay_norm1)

        def project(weight_mat):
            projected = jnp.dot(normed, weight_mat, preferred_element_type=jnp.float32).astype(jnp.bfloat16)
            return projected.reshape(BATCH_SIZE, SEQ_LEN, NUM_HEADS, HEAD_DIM).transpose(2, 0, 1, 3)

        context = lax.map(head_attn, (project(lay_query), project(lay_key), project(lay_value), dist_table.T))
        context = context.transpose(1, 2, 0, 3).reshape(token_rows, INNER_DIM)
        attn_out = jnp.dot(context, lay_out, preferred_element_type=jnp.float32)
        mid_resid = (residual.astype(jnp.float32) + attn_out).astype(jnp.bfloat16)
        normed_mlp = rms_norm(mid_resid, lay_norm2)
        act_proj = jnp.dot(normed_mlp, lay_act, preferred_element_type=jnp.float32)
        lin_proj = jnp.dot(normed_mlp, lay_lin, preferred_element_type=jnp.float32)
        gated = (jax.nn.gelu(act_proj, approximate=True) * lin_proj).astype(jnp.bfloat16)
        ffn_out = jnp.dot(gated, lay_down, preferred_element_type=jnp.float32)
        return (mid_resid.astype(jnp.float32) + ffn_out).astype(jnp.bfloat16), None

    stacked = (w_query, w_key, w_value, w_out, w_act, w_lin, w_down, norm_attn, norm_mlp)
    final_rows, no_out = lax.scan(layer, tokens.reshape(token_rows, MODEL_DIM), stacked)
    return final_rows.reshape(BATCH_SIZE, SEQ_LEN, MODEL_DIM)
```

```python
import functools

import jax
import jax.numpy as jnp
from jax import lax
from jax.experimental import pallas as pl
from jax.experimental.pallas import tpu as pltpu
from jax.sharding import PartitionSpec as P

QT = 128


def rel_bucket(offsets):
    side = jnp.where(offsets > 0, 16, 0)
    distance = jnp.minimum(jnp.abs(offsets), 128)
    limits = 64 * 2 ** jnp.arange(1, 8)
    steps = jnp.sum((distance[..., None] * distance[..., None] >= limits).astype(jnp.int32), axis=-1)
    return side + jnp.where(distance < 8, distance, 8 + steps)


def rms_norm(rows_in, gain_vec):
    rows32 = rows_in.astype(jnp.float32)
    inv_rms = lax.rsqrt(jnp.mean(rows32 * rows32, axis=-1, keepdims=True) + 1e-6)
    return (rows32 * inv_rms * gain_vec).astype(jnp.bfloat16)


def bias_strips(rel_table, seq_len):
    width = 2 * seq_len - QT
    rows = lax.broadcasted_iota(jnp.int32, (QT, width), 0)
    cols = lax.broadcasted_iota(jnp.int32, (QT, width), 1)
    bucket = rel_bucket(cols - rows - (seq_len - QT))
    one_hot = (bucket[None] == lax.broadcasted_iota(jnp.int32, (rel_table.shape[0], QT, width), 0)).astype(jnp.float32)
    return jnp.einsum('bh,brc->hrc', rel_table, one_hot, precision=lax.Precision.HIGHEST)


def attn_kernel(q_ref, k_ref, v_ref, strip_ref, mask_ref, o_ref):
    seq_len = q_ref.shape[0]
    keys = k_ref[...]
    vals = v_ref[...]
    mask = mask_ref[...]
    low = lax.broadcasted_iota(jnp.int32, (QT, 128), 1) < 64

    def tile(i, carry):
        q = q_ref[pl.ds(pl.multiple_of(i * QT, QT), QT), :]
        start = pl.multiple_of(seq_len - QT - i * QT, QT)
        outs = []
        for h in range(2):
            qh = jnp.where(low if h == 0 else jnp.logical_not(low), q, jnp.zeros_like(q))
            s = lax.dot_general(qh, keys, (((1,), (1,)), ((), ())), preferred_element_type=jnp.float32)
            s = s + strip_ref[h, :, pl.ds(start, seq_len)] + mask
            e = jnp.exp(s - jnp.max(s, axis=1, keepdims=True))
            p = (e * (1.0 / jnp.sum(e, axis=1, keepdims=True))).astype(jnp.bfloat16)
            outs.append(jnp.dot(p, vals, preferred_element_type=jnp.float32))
        o_ref[pl.ds(pl.multiple_of(i * QT, QT), QT), :] = jnp.where(low, outs[0], outs[1]).astype(jnp.bfloat16)
        return carry

    lax.fori_loop(0, seq_len // QT, tile, 0)


def attention(q, k, v, strips, mask):
    seq_len, width = q.shape
    pairs = width // 128
    head_block = pl.BlockSpec((seq_len, 128), lambda h: (0, h))
    return pl.pallas_call(
        attn_kernel,
        grid=(pairs,),
        in_specs=[head_block, head_block, head_block,
                  pl.BlockSpec((2, QT, strips.shape[2]), lambda h: (h, 0, 0)),
                  pl.BlockSpec((1, seq_len), lambda h: (0, 0))],
        out_specs=head_block,
        out_shape=jax.ShapeDtypeStruct((seq_len, width), jnp.bfloat16),
        compiler_params=pltpu.CompilerParams(dimension_semantics=('arbitrary',)),
        cost_estimate=pl.CostEstimate(flops=16 * seq_len * seq_len * width, bytes_accessed=8 * seq_len * width,
                                      transcendentals=seq_len * seq_len * 2 * pairs),
        name='attn',
    )(q, k, v, strips, mask)


def solution(mesh):
    group_size = mesh.shape['tp']
    col_spec = P(None, None, 'tp')
    row_spec = P(None, 'tp', None)

    def local_fn(tokens, pad_mask, rel_table, w_query, w_key, w_value, w_out, w_act, w_lin, w_down, norm_attn, norm_mlp):
        batch, seq_loc, model_dim = tokens.shape
        seq_len = seq_loc * group_size
        strips = bias_strips(rel_table, seq_len)
        key_bias = jnp.where(pad_mask == 1, 0.0, -1e9).astype(jnp.float32)

        def mm(a, b):
            return jnp.dot(a, b, preferred_element_type=jnp.float32)

        def entry(resid, gain):
            normed = []
            for s in range(batch):
                if s:
                    resid[s], _ = lax.optimization_barrier((resid[s], normed[s - 1]))
                normed.append(rms_norm(resid[s], gain))
            return [lax.all_gather(n, 'tp', axis=0, tiled=True) for n in normed]

        resid = [tokens[s] for s in range(batch)]
        for layer in range(w_query.shape[0]):
            gathered = entry(resid, norm_attn[layer])
            for s in range(batch):
                h = gathered[s]
                q, k, v = (mm(h, w[layer]).astype(jnp.bfloat16) for w in (w_query, w_key, w_value))
                ctx = attention(q, k, v, strips, key_bias[s:s + 1])
                part = mm(ctx, w_out[layer]).astype(jnp.bfloat16)
                red = lax.psum_scatter(part, 'tp', scatter_dimension=0, tiled=True)
                resid[s] = (resid[s].astype(jnp.float32) + red.astype(jnp.float32)).astype(jnp.bfloat16)
            gathered = entry(resid, norm_mlp[layer])
            for s in range(batch):
                h = gathered[s]
                act = jax.nn.gelu(mm(h, w_act[layer]), approximate=True)
                gated = (act * mm(h, w_lin[layer])).astype(jnp.bfloat16)
                part = mm(gated, w_down[layer]).astype(jnp.bfloat16)
                red = lax.psum_scatter(part, 'tp', scatter_dimension=0, tiled=True)
                resid[s] = (resid[s].astype(jnp.float32) + red.astype(jnp.float32)).astype(jnp.bfloat16)
        return jnp.stack(resid)

    in_specs = (P('dp', 'tp', None), P('dp', None), P(None, 'tp'), col_spec, col_spec, col_spec, row_spec,
                col_spec, col_spec, row_spec, P(None, None), P(None, None))
    return jax.shard_map(local_fn, mesh=mesh, in_specs=in_specs, out_specs=P('dp', 'tp', None), check_vma=False)
```

```python
import functools

import jax
import jax.numpy as jnp
from jax import lax
from jax.experimental import pallas as pl
from jax.experimental.pallas import tpu as pltpu
from jax.sharding import PartitionSpec as P

MESH = pl.DeviceIdType.MESH
CORES = 2
BIAS_BLOCKS = 5
ROWS = 16


def rel_bucket(offsets):
    side = jnp.where(offsets > 0, 16, 0)
    distance = jnp.minimum(jnp.abs(offsets), 128)
    steps = jnp.zeros_like(offsets)
    for octave in range(1, 8):
        steps += (distance * distance >= 64 * 2 ** octave).astype(jnp.int32)
    return side + jnp.where(distance < 8, distance, 8 + steps)


def bias_blocks(table_ref, bias_ref):
    heads, block, _ = bias_ref.shape

    def step(n, carry):
        d, r = lax.rem(n, BIAS_BLOCKS), lax.div(n, BIAS_BLOCKS) * ROWS
        rows = lax.broadcasted_iota(jnp.int32, (ROWS, block), 0) + r
        cols = lax.broadcasted_iota(jnp.int32, (ROWS, block), 1) + (d - BIAS_BLOCKS // 2) * block
        bucket = rel_bucket(cols - rows)
        values = [jnp.full((ROWS, block), table_ref[0, h], jnp.float32) for h in range(heads)]
        for k in range(1, table_ref.shape[0]):
            hit = bucket == k
            values = [jnp.where(hit, table_ref[k, h], values[h]) for h in range(heads)]
        for h in range(heads):
            bias_ref[h, rows_of(r, ROWS), pl.ds(pl.multiple_of(d * block, 128), block)] = values[h]
        return carry

    lax.fori_loop(0, BIAS_BLOCKS * (block // ROWS), step, 0)


def rows_of(start, count):
    return pl.ds(pl.multiple_of(start, ROWS), count)


class Block:
    def __init__(self, chips, layer, x_ref, gain_ref, out_ref, held, pair_in, half_in, full_in, ag_send, ag_recv, rs_send, rs_recv):
        me = lax.axis_index('tp')
        self.chips, self.layer = chips, layer
        self.x_ref, self.gain_ref, self.out_ref, self.held = x_ref, gain_ref, out_ref, held
        self.pair_in, self.half_in, self.full_in = pair_in, half_in, full_in
        self.ag_send, self.ag_recv, self.rs_send, self.rs_recv = ag_send, ag_recv, rs_send, rs_recv
        self.chip, self.core = lax.div(me, CORES), lax.rem(me, CORES)
        self.blk, self.half = x_ref.shape[1], x_ref.shape[1] // 2
        self.right = lax.rem(self.chip + 1, chips)
        self.opp = lax.rem(self.chip + 2, chips)
        self.left = lax.rem(self.chip + 3, chips)
        self.dev_right = self.right * CORES + self.core
        self.dev_left = self.left * CORES + self.core
        self.other = 1 - self.core
        self.partner = self.chip * CORES + self.other

    def barrier(self):
        sem = pltpu.get_barrier_semaphore()
        for dev in (self.dev_left, self.dev_right, self.partner):
            pl.semaphore_signal(sem, inc=1, device_id={'tp': dev}, device_id_type=MESH)
        pl.semaphore_wait(sem, 3)

    def token_rows(self, chip, core, part=None):
        start = (chip * CORES + core) * self.blk
        if part is None:
            return rows_of(start, self.blk)
        return rows_of(start + part * self.half, self.half)

    def norm(self, s):
        own = (self.chip * CORES + self.core) * self.blk

        def step(i, carry):
            x = self.x_ref[s, rows_of(i * ROWS, ROWS), :].astype(jnp.float32)
            inv = lax.rsqrt(jnp.mean(x * x, axis=-1, keepdims=True) + 1e-6)
            self.held[s, rows_of(own + i * ROWS, ROWS), :] = (x * inv * self.gain_ref[self.layer:self.layer + 1, :]).astype(jnp.bfloat16)
            return carry

        lax.fori_loop(0, self.blk // ROWS, step, 0)

    def _ag(self, s, k, rows, dev):
        ref = self.held.at[s, rows]
        return pltpu.make_async_remote_copy(src_ref=ref, dst_ref=ref, send_sem=self.ag_send.at[s, k],
                                            recv_sem=self.ag_recv.at[s, k], device_id={'tp': dev}, device_id_type=MESH)

    def ag_copy(self, s, k):
        c = self.core
        rows = (lambda: self.token_rows(self.chip, c, 0), lambda: self.token_rows(self.chip, c, 1),
                lambda: self.token_rows(self.chip, c, 1), lambda: self.token_rows(self.chip, c, 0),
                lambda: self.token_rows(self.left, c, 0), lambda: self.token_rows(self.right, c, 1),
                lambda: self.token_rows(self.chip, c), lambda: self.token_rows(self.left, c),
                lambda: self.token_rows(self.right, c), lambda: self.token_rows(self.opp, c))[k]()
        dev = (self.dev_right, self.dev_right, self.dev_left, self.dev_left, self.dev_right, self.dev_left,
               self.partner, self.partner, self.partner, self.partner)[k]
        return self._ag(s, k, rows, dev)

    def ag_wait(self, s, *which):
        c, o = self.core, self.other
        rows = [self.token_rows(self.left, c, 0), self.token_rows(self.left, c, 1), self.token_rows(self.right, c, 1),
                self.token_rows(self.right, c, 0), self.token_rows(self.opp, c, 0), self.token_rows(self.opp, c, 1),
                self.token_rows(self.chip, o), self.token_rows(self.left, o), self.token_rows(self.right, o),
                self.token_rows(self.opp, o)]
        for k in which:
            self._ag(s, k, rows[k], self.partner).wait_recv()

    def ag_start(self, s):
        for k in (0, 2, 1, 3):
            self.ag_copy(s, k).start()

    def ag_forward(self, s):
        self.ag_wait(s, 0)
        self.ag_copy(s, 4).start()
        self.ag_wait(s, 2)
        self.ag_copy(s, 5).start()

    def ag_share(self, s):
        self.ag_wait(s, 1)
        self.ag_copy(s, 7).start()
        self.ag_wait(s, 3)
        self.ag_copy(s, 8).start()

    def ag_share_opp(self, s):
        self.ag_wait(s, 4, 5)
        self.ag_copy(s, 9).start()

    def ag_drain(self, s):
        for k in range(10):
            self.ag_copy(s, k).wait_send()

    def _rs(self, s, k, rows, dst, dev):
        return pltpu.make_async_remote_copy(src_ref=self.held.at[s, rows], dst_ref=dst, send_sem=self.rs_send.at[s, k],
                                            recv_sem=self.rs_recv.at[s, k], device_id={'tp': dev}, device_id_type=MESH)

    def rs_copy(self, s, k):
        c, o, h = self.core, self.other, self.half
        lo, hi = pl.ds(0, h), pl.ds(h, h)
        if k < 4:
            chip = (self.opp, self.right, self.left, self.chip)[k]
            return self._rs(s, k, self.token_rows(chip, o), self.pair_in.at[s, k], self.partner)
        chip, part, dst = ((self.opp, 0, self.half_in.at[s, 0]), (self.opp, 1, self.half_in.at[s, 1]),
                           (self.right, 1, self.full_in.at[s, 0, hi]), (self.left, 0, self.full_in.at[s, 1, lo]),
                           (self.right, 0, self.full_in.at[s, 0, lo]), (self.left, 1, self.full_in.at[s, 1, hi]))[k - 4]
        return self._rs(s, k, self.token_rows(chip, c, part), dst, self.dev_left if k % 2 else self.dev_right)

    def rs_pair(self, s, *which):
        for k in which:
            self.rs_copy(s, k).start()

    def _add(self, s, start, count, other):
        def step(i, carry):
            at = rows_of(start + i * ROWS, ROWS)
            total = self.held[s, at, :].astype(jnp.float32) + other(rows_of(i * ROWS, ROWS)).astype(jnp.float32)
            self.held[s, at, :] = total.astype(jnp.bfloat16)
            return carry

        lax.fori_loop(0, count // ROWS, step, 0)

    def rs_first(self, s, *which):
        for k in which:
            chip, then = ((self.opp, (4, 5)), (self.right, (6,)), (self.left, (7,)), (self.chip, ()))[k]
            self.rs_copy(s, k).wait_recv()
            self._add(s, (chip * CORES + self.core) * self.blk, self.blk, lambda at: self.pair_in[s, k, at, :])
            for j in then:
                self.rs_copy(s, j).start()

    def rs_second(self, s):
        for k, chip, part in ((4, self.right, 0), (5, self.left, 1)):
            self.rs_copy(s, k).wait_recv()
            start = (chip * CORES + self.core) * self.blk + part * self.half
            self._add(s, start, self.half, lambda at: self.half_in[s, part, at, :])
            self.rs_copy(s, k + 4).start()

    def rs_last(self, s):
        for k in (6, 7, 8, 9):
            self.rs_copy(s, k).wait_recv()
        own = (self.chip * CORES + self.core) * self.blk

        def step(i, carry):
            at = rows_of(i * ROWS, ROWS)
            total = self.held[s, rows_of(own + i * ROWS, ROWS), :].astype(jnp.float32)
            total = total + self.full_in[s, 0, at, :].astype(jnp.float32) + self.full_in[s, 1, at, :].astype(jnp.float32)
            self.out_ref[s, at, :] = (self.x_ref[s, at, :].astype(jnp.float32) + total).astype(jnp.bfloat16)
            return carry

        lax.fori_loop(0, self.blk // ROWS, step, 0)

    def rs_drain(self, s):
        for k in range(10):
            self.rs_copy(s, k).wait_send()


def run_block(b, first, middle, second, prepare, early, restore):
    def tail(s, between):
        second(s, (b.opp, b.right), 0)
        second(s, (b.opp, b.right), 1)
        b.rs_pair(s, 0, 1)
        between()
        second(s, (b.left, b.chip), 0)
        b.rs_first(s, 0, 1)
        second(s, (b.left, b.chip), 1)
        b.rs_pair(s, 2, 3)

    b.barrier()
    prepare()
    b.norm(0)
    b.ag_start(0)
    b.ag_copy(0, 6).start()
    b.norm(1)
    b.ag_copy(1, 6).start()
    early()
    b.ag_wait(0, 6)
    first(0, b.chip)
    b.ag_wait(1, 6)
    first(1, b.chip, True)
    b.ag_forward(0)
    b.ag_start(1)
    b.ag_share(0)
    b.ag_wait(0, 7)
    first(0, b.left)
    b.ag_wait(0, 8)
    first(0, b.right)
    b.ag_share_opp(0)
    b.ag_wait(0, 9)
    first(0, b.opp)
    middle(0, lambda: b.ag_forward(1))
    b.ag_drain(0)
    tail(0, lambda: None)
    b.ag_share(1)
    b.rs_first(0, 2, 3)
    restore()
    b.ag_share_opp(1)
    b.ag_wait(1, 7)
    first(1, b.left)
    b.ag_wait(1, 8)
    first(1, b.right)
    b.ag_wait(1, 9)
    first(1, b.opp)
    middle(1, lambda: b.rs_second(0))
    b.ag_drain(1)
    tail(1, lambda: None)
    b.rs_first(1, 2, 3)
    b.rs_last(0)
    b.rs_drain(0)
    b.rs_second(1)
    b.rs_last(1)
    b.rs_drain(1)


def attn_kernel(chips, layer, x_ref, gain_ref, table_ref, pad_ref, wq_ref, wk_ref, wv_ref, wo_ref, out_ref,
                held, pair_in, half_in, full_in, w_in, w_back, proj, ctx, bias_ref, mask_ref, score_a, score_b, probs_ref, w_sem, ag_send, ag_recv, rs_send, rs_recv):
    b = Block(chips, layer, x_ref, gain_ref, out_ref, held, pair_in, half_in, full_in, ag_send, ag_recv, rs_send, rs_recv)
    seq_len, model_dim = held.shape[1], held.shape[2]
    width = proj.shape[2]
    blk = b.blk
    chip_rows = CORES * blk
    blocks = seq_len // blk
    score_refs = (score_a, score_b)
    loads = [pltpu.make_async_copy(w.at[layer], w_in.at[j], w_sem.at[j]) for j, w in enumerate((wq_ref, wk_ref, wv_ref))]
    load_out = pltpu.make_async_copy(wo_ref.at[layer], w_back, w_sem.at[3])

    def prepare():
        for load in loads + [load_out]:
            load.start()

    started = []

    def early():
        bias_blocks(table_ref, bias_ref)
        mask_ref[...] = jnp.where(pad_ref[...] == 1, 0.0, -1e9).astype(jnp.float32)

    def restore():
        def step(j, carry):
            proj[j, rows_of(b.chip * chip_rows, chip_rows), :] = proj[j, seq_len:, :]
            return carry

        lax.fori_loop(0, 3, step, 0)

    def first(s, chip, aside=False):
        if not started:
            started.append(0)
            for load in loads:
                load.wait()
        rows = rows_of(chip * chip_rows, chip_rows)
        to = pl.ds(seq_len, chip_rows) if aside else rows

        def step(j, carry):
            product = jnp.dot(held[s, rows, :], w_in[j], preferred_element_type=jnp.float32)
            proj[j, to, :] = product.astype(jnp.bfloat16)
            return carry

        lax.fori_loop(0, 3, step, 0)

    low = lax.broadcasted_iota(jnp.int32, (chip_rows, 128), 1) < 64

    group = 32

    def scores_of(n, slot):
        pair, i = lax.div(n, chips), lax.rem(n, chips)
        cols = pl.ds(pl.multiple_of(pair * 128, 128), 128)
        q = proj[0, rows_of(i * chip_rows, chip_rows), cols]
        zero = jnp.zeros_like(q)
        both = jnp.concatenate([jnp.where(low, q, zero), jnp.where(low, zero, q)], axis=0)
        score_refs[slot][...] = lax.dot_general(both, proj[1, :seq_len, cols], (((1,), (1,)), ((), ())),
                                                preferred_element_type=jnp.float32)

    def attend(s, n, slot):
        pair, i = lax.div(n, chips), lax.rem(n, chips)
        cols = pl.ds(pl.multiple_of(pair * 128, 128), 128)
        mask = mask_ref[pl.ds(s, 1), :]
        for part in range(2 * CORES):
            h, sub = part // CORES, part % CORES
            at = [(jnp.clip(j - i * CORES - sub, -(BIAS_BLOCKS // 2), BIAS_BLOCKS // 2) + BIAS_BLOCKS // 2) * blk
                  for j in range(blocks)]
            for r in range(0, blk, group):
                pieces = [score_refs[slot][part * blk + r:part * blk + r + group, j * blk:(j + 1) * blk]
                          + bias_ref[pair * 2 + h, r:r + group, pl.ds(pl.multiple_of(at[j], 128), blk)]
                          + mask[:, j * blk:(j + 1) * blk] for j in range(blocks)]
                full = jnp.concatenate(pieces, axis=1)
                e = jnp.exp(full - jnp.max(full, axis=1, keepdims=True))
                probs_ref[part * blk + r:part * blk + r + group, :] = (
                    e * (1.0 / jnp.sum(e, axis=1, keepdims=True))).astype(jnp.bfloat16)
        outs = jnp.dot(probs_ref[...], proj[2, :seq_len, cols], preferred_element_type=jnp.float32)
        ctx[rows_of(i * chip_rows, chip_rows), cols] = jnp.where(low, outs[:chip_rows], outs[chip_rows:]).astype(jnp.bfloat16)

    def middle(s, hook):
        count = (width // 128) * chips
        scores_of(0, 0)

        def step(m, carry):
            n = 2 * m
            scores_of(n + 1, 1)
            attend(s, n, 0)
            scores_of(jnp.minimum(n + 2, count - 1), 0)
            attend(s, n + 1, 1)
            return carry

        lax.fori_loop(0, count // 4, step, 0)
        hook()
        lax.fori_loop(count // 4, count // 2, step, 0)
        if s == 0:
            load_out.wait()

    tile = 512

    def second(s, which, part):
        tiles = model_dim // tile

        def step(n, carry):
            cols = pl.ds(pl.multiple_of(n * tile, tile), tile)
            for chip in which:
                rows = rows_of(chip * chip_rows, chip_rows)
                held[s, rows, cols] = jnp.dot(ctx[rows, :], w_back[:, cols], preferred_element_type=jnp.float32).astype(jnp.bfloat16)
            return carry

        lax.fori_loop(part * tiles // 2, (part + 1) * tiles // 2, step, 0)

    run_block(b, first, middle, second, prepare, early, restore)


def ffn_kernel(chips, layer, x_ref, gain_ref, wa_ref, wl_ref, wd_ref, out_ref,
               held, pair_in, half_in, full_in, w_in, w_back, gated, w_sem, d_sem, ag_send, ag_recv, rs_send, rs_recv):
    b = Block(chips, layer, x_ref, gain_ref, out_ref, held, pair_in, half_in, full_in, ag_send, ag_recv, rs_send, rs_recv)
    model_dim = held.shape[2]
    seq_len, width = held.shape[1], gated.shape[1]
    blk = b.blk
    chip_rows = CORES * blk
    tile_in, tile_out = 256, w_back.shape[2]
    loads = [pltpu.make_async_copy(w.at[layer, :, pl.ds(n * tile_in, tile_in)],
                                   w_in.at[n, :, pl.ds(half * tile_in, tile_in)], w_sem.at[2 * n + half])
             for n in range(width // tile_in) for half, w in enumerate((wa_ref, wl_ref))]

    def prepare():
        for load in loads:
            load.start()

    started = []

    def restore():
        gated[rows_of(b.chip * chip_rows, chip_rows), :] = gated[seq_len:, :]

    def first(s, chip, aside=False):
        if not started:
            started.append(0)
            for load in loads:
                load.wait()
        rows = rows_of(chip * chip_rows, chip_rows)
        to = pl.ds(seq_len, chip_rows) if aside else rows

        def step(n, carry):
            cols = pl.ds(pl.multiple_of(n * tile_in, tile_in), tile_in)
            both = jnp.dot(held[s, rows, :], w_in[n], preferred_element_type=jnp.float32)
            act, lin = both[:, :tile_in], both[:, tile_in:]
            gated[to, cols] = (jax.nn.gelu(act, approximate=True) * lin).astype(jnp.bfloat16)
            return carry

        lax.fori_loop(0, width // tile_in, step, 0)

    tiles = model_dim // tile_out

    def load_back(n):
        cols = pl.ds(pl.multiple_of(n * tile_out, tile_out), tile_out)
        slot = lax.rem(n, 2)
        return pltpu.make_async_copy(wd_ref.at[layer, :, cols], w_back.at[slot], d_sem.at[slot])

    def second(s, which, part):
        if part == 0:
            load_back(0).start()

        def step(n, carry):
            @pl.when(n + 1 < tiles)
            def _():
                load_back(n + 1).start()

            load_back(n).wait()
            cols = pl.ds(pl.multiple_of(n * tile_out, tile_out), tile_out)
            for chip in which:
                rows = rows_of(chip * chip_rows, chip_rows)
                product = jnp.dot(gated[rows, :], w_back[lax.rem(n, 2)], preferred_element_type=jnp.float32)
                held[s, rows, cols] = product.astype(jnp.bfloat16)
            return carry

        lax.fori_loop(part * tiles // 2, (part + 1) * tiles // 2, step, 0)

    run_block(b, first, lambda s, hook: hook(), second, prepare, lambda: None, restore)


def comm_scratch(batch, seq_len, blk, dim):
    chips = seq_len // (CORES * blk)
    return [pltpu.VMEM((batch, seq_len, dim), jnp.bfloat16), pltpu.VMEM((batch, chips, blk, dim), jnp.bfloat16),
            pltpu.VMEM((batch, 2, blk // 2, dim), jnp.bfloat16), pltpu.VMEM((batch, 2, blk, dim), jnp.bfloat16)]


def comm_sems(batch):
    return [pltpu.SemaphoreType.DMA((batch, 10))] * 4


def call_block(kernel, name, cid, x, operands, extra, sems, flops, placed):
    batch, blk, dim = x.shape
    spaces = (pl.BlockSpec(memory_space=pl.ANY), pl.BlockSpec(memory_space=pltpu.VMEM), pl.BlockSpec(memory_space=pltpu.SMEM))
    seq_len = extra[0]
    return pl.pallas_call(
        kernel,
        out_shape=jax.ShapeDtypeStruct(x.shape, x.dtype),
        in_specs=[spaces[1]] + [spaces[where] for where in placed],
        out_specs=spaces[1],
        scratch_shapes=comm_scratch(batch, seq_len, blk, dim) + extra[1] + sems + comm_sems(batch),
        compiler_params=pltpu.CompilerParams(collective_id=cid, has_side_effects=True, vmem_limit_bytes=67_000_000),
        cost_estimate=pl.CostEstimate(flops=flops, bytes_accessed=0, transcendentals=0),
        name=name,
    )(x, *operands)


def solution(mesh):
    group_size = mesh.shape['tp']
    chips = group_size // CORES
    col_spec = P(None, None, 'tp')
    row_spec = P(None, 'tp', None)

    def local_fn(tokens, pad_mask, rel_table, w_query, w_key, w_value, w_out, w_act, w_lin, w_down, norm_attn, norm_mlp):
        batch, blk, dim = tokens.shape
        seq_len = blk * group_size
        width, ff = w_query.shape[2], w_act.shape[2]
        x = tokens
        for layer in range(w_query.shape[0]):
            x = call_block(
                functools.partial(attn_kernel, chips, layer), 'attn_block', 2 * layer, x,
                (norm_attn, rel_table, pad_mask, w_query, w_key, w_value, w_out),
                (seq_len, [pltpu.VMEM((3, dim, width), jnp.bfloat16), pltpu.VMEM((width, dim), jnp.bfloat16),
                           pltpu.VMEM((3, seq_len + CORES * blk, width), jnp.bfloat16), pltpu.VMEM((seq_len, width), jnp.bfloat16),
                           pltpu.VMEM((rel_table.shape[1], blk, BIAS_BLOCKS * blk), jnp.float32), pltpu.VMEM((batch, seq_len), jnp.float32),
                           pltpu.VMEM((2 * CORES * blk, seq_len), jnp.float32), pltpu.VMEM((2 * CORES * blk, seq_len), jnp.float32),
                           pltpu.VMEM((2 * CORES * blk, seq_len), jnp.bfloat16)]),
                [pltpu.SemaphoreType.DMA((4,))], 8 * batch * seq_len * dim * width, (1, 2, 1, 0, 0, 0, 0))
            x = call_block(
                functools.partial(ffn_kernel, chips, layer), 'ffn_block', 2 * layer + 1, x,
                (norm_mlp, w_act, w_lin, w_down),
                (seq_len, [pltpu.VMEM((ff // 256, dim, 512), jnp.bfloat16),
                           pltpu.VMEM((2, ff, 512), jnp.bfloat16), pltpu.VMEM((seq_len + CORES * blk, ff), jnp.bfloat16)]),
                [pltpu.SemaphoreType.DMA((2 * (ff // 256),)), pltpu.SemaphoreType.DMA((2,))], 6 * batch * seq_len * dim * ff, (1, 0, 0, 0))
        return x

    in_specs = (P('dp', 'tp', None), P('dp', None), P(None, 'tp'), col_spec, col_spec, col_spec, row_spec,
                col_spec, col_spec, row_spec, P(None, None), P(None, None))
    return jax.shard_map(local_fn, mesh=mesh, in_specs=in_specs, out_specs=P('dp', 'tp', None), check_vma=False)
```
